256 devices in a mesh: samp: 32 (over z, y_hi, core), snp: 8 (over y_lo, x).
Axes of the slice: x: 4, y: 4 (y_hi: 2, y_lo: 2; y = y_hi * 2 + y_lo), z: 8, core: 2. Of those that a mesh axis runs over, the one named last changes fastest.
Arguments:
- genotypes: float32 [8192, 8192], P('samp', 'snp'), may hold values from 0 to 2, as said below
- observed: int32 [8192, 8192], P('samp', 'snp'), may hold values from 0 to 1
Outputs:
- relation: float32 [32, 8, 32, 8192], P(None, 'snp', None, 'samp')
The draws below stay inside these ranges and needn't reach their ends.
Inputs may be any that keep to these rules, and one draw needn't show every extreme that they name: `genotypes`: dosages are real numbers between 0 and 2.
All inputs are finite; a program needn't handle non-finite values.
Results may differ from the reference program's by a relative error of at most 0.00061.
Values may be sent and summed in bfloat16 or wider, within the bound.
No kernel may reach another device: no remote copies, remote signals or barrier semaphores. Data moves between devices by JAX's collectives and lax.ppermute only.
A program may use at most 128 MiB of HBM per device.

```python
import jax
import jax.numpy as jnp
from jax import lax

SAMPLES = 8192
SNPS = 8192
TILE = 32
N_SAMP = 32
N_SNP = 8


def soft_allele(key, threshold, error_top):
    hard_key = jax.random.fold_in(key, 1)
    error_key = jax.random.fold_in(key, 2)
    carried = jax.random.uniform(hard_key, threshold.shape, jnp.float32) < threshold
    error = jax.random.uniform(error_key, threshold.shape, jnp.float32) * error_top
    return jnp.where(carried, 1.0 - error, error)


def draw_genotypes(key, part):
    rate_key = jax.random.fold_in(key, 11)
    first_key = jax.random.fold_in(key, 12)
    second_key = jax.random.fold_in(key, 13)
    base_rate = jax.random.uniform(rate_key, (SNPS,), jnp.float32, 0.005, 0.331)
    position = (jnp.arange(SAMPLES, dtype=jnp.float32) / SAMPLES)[:, None]
    threshold = base_rate[None, :] * (1.0 + 2.0 * position)
    first_allele = soft_allele(first_key, threshold, 0.3)
    second_allele = soft_allele(second_key, threshold, 0.3)
    return jnp.clip(first_allele + second_allele, 0.0, 2.0).astype(jnp.float32)


def draw_observed(key, part):
    shift_key = jax.random.fold_in(key, 21)
    call_key = jax.random.fold_in(key, 22)
    snp_shift = jax.random.randint(shift_key, (SNPS,), 0, 40)
    sample_index = jnp.arange(SAMPLES, dtype=jnp.int32)
    threshold = 500 + 480 * sample_index[:, None] // SAMPLES - snp_shift[None, :]
    call_draw = jax.random.randint(call_key, (SAMPLES, SNPS), 0, 1000)
    return (call_draw < threshold).astype(jnp.int32)


def setup_inputs(seed: int = 0) -> dict:
    key_of = jax.random.split(jax.random.key(seed), 3)
    return {
        "genotypes": draw_genotypes(jax.random.fold_in(key_of[2], 71), 0),
        "observed": draw_observed(jax.random.fold_in(key_of[2], 71), 0),
    }


var_floor = 0.1

def reference(genotypes, observed):
    present = observed.astype(jnp.float32)
    dosage = genotypes.astype(jnp.float32)
    alt_sum = lax.optimization_barrier(jnp.sum(present * dosage, axis=0))
    call_sum = lax.optimization_barrier(jnp.sum(present, axis=0))
    frequency = alt_sum / (2.0 * jnp.maximum(call_sum, 1.0))
    variance = jnp.maximum(2.0 * frequency * (1.0 - frequency), var_floor)
    scaled = (present * (dosage - 2.0 * frequency) * lax.rsqrt(variance)).astype(jnp.bfloat16)
    widened = scaled.astype(jnp.float32)
    grm = jnp.dot(widened, widened.T, precision=lax.Precision.HIGHEST) / SNPS
    return grm.reshape(N_SAMP, N_SNP, TILE, SAMPLES)
```

```python
import jax
import jax.numpy as jnp
from jax import lax
from jax.sharding import Mesh, PartitionSpec as P

var_floor = 0.1
SAMP = ("z", "yh", "core")
SNP = ("yl", "x")
FLIP = [(0, 1), (1, 0)]


def from_everyone(x, axis):
    devices = lax.axis_size(axis)
    return lax.all_to_all(jnp.broadcast_to(x[None], (devices, *x.shape)), axis, 0, 0, tiled=True)


def shift(x, axis, by):
    n = lax.axis_size(axis)
    return lax.ppermute(x, axis, [(i, (i + by) % n) for i in range(n)])


def scale(genotypes, observed):
    present = observed.astype(jnp.float32)
    alt_local = jnp.sum(present * genotypes, axis=0)
    call_local = jnp.sum(present, axis=0)
    snps = alt_local.shape[0]
    total = jnp.sum(from_everyone(jnp.concatenate([alt_local, call_local]), SAMP), axis=0)
    alt_sum, call_sum = total[:snps], total[snps:]
    frequency = alt_sum / (2.0 * jnp.maximum(call_sum, 1.0))
    variance = jnp.maximum(2.0 * frequency * (1.0 - frequency), var_floor)
    return (present * (genotypes - 2.0 * frequency) * lax.rsqrt(variance)).astype(jnp.bfloat16)


def flip_y(x, yh, yl):
    pairs = [(h * 2 + l, (h ^ yh) * 2 + (l ^ yl)) for h in range(2) for l in range(2)]
    return lax.ppermute(x, ("yh", "yl"), pairs)


def ring(streams):
    got = {0: list(streams)}
    n = lax.axis_size("z")
    for by in range(1, n // 2 + 1):
        for s in (0, 1):
            if by < n // 2 or s == 0:
                got.setdefault(-by, [None, None])[s] = shift(got[1 - by][s], "z", 1)
            if by < n // 2 or s == 1:
                got.setdefault(by, [None, None])[s] = shift(got[by - 1][s], "z", -1)
    far = n // 2
    last = got.pop(-far)
    got[far][0] = last[0]
    return got


def body(genotypes, observed):
    z, yh, core, yl, x = (lax.axis_index(a) for a in ("z", "yh", "core", "yl", "x"))
    rows, snps = genotypes.shape
    classes = lax.axis_size("x")
    tile = rows // lax.axis_size(SNP)
    scaled = scale(genotypes, observed)
    half = rows // 2
    mine = lax.dynamic_slice_in_dim(scaled, yl * half, half, 0)
    theirs = lax.dynamic_slice_in_dim(scaled, (1 - yl) * half, half, 0)
    from_pair_mine = flip_y(theirs, 0, 1)
    from_pair_other = flip_y(mine, 0, 1)

    def by_class(block):
        doubled = jnp.concatenate([block, block], axis=0)
        return lax.dynamic_slice_in_dim(doubled, x * tile, half, 0)

    held = ring((by_class(mine), by_class(from_pair_mine)))
    low = jnp.where(yl == 0, from_pair_mine, from_pair_other)
    high = jnp.where(yl == 0, from_pair_other, from_pair_mine)
    pair = jnp.concatenate([low, high], axis=0)
    own = jnp.concatenate([scaled, pair], axis=1)
    across = jnp.concatenate([flip_y(scaled, 1, 0), flip_y(scaled, 1, 1)], axis=1)
    cols = jnp.concatenate([own, lax.ppermute(own, "core", FLIP), across, lax.ppermute(across, "core", FLIP)], axis=0)

    done = {}
    for group in ((0, 1, -1), (2, -2), (3, -3, 4)):
        left = jnp.concatenate([jnp.concatenate(held[d], axis=1) for d in group], axis=0)
        part = lax.dot_general(left, cols, (((1,), (1,)), ((), ())), preferred_element_type=jnp.float32)
        part = part.reshape(len(group), classes, tile, -1)
        total = part[:, 0]
        for j in range(1, classes):
            total = total + shift(part[:, j], "x", j)
        total = total / (snps * lax.axis_size(SNP))
        quarter = [total[..., b * rows:(b + 1) * rows] for b in range(4)]
        quarter[1] = lax.ppermute(quarter[1], "core", FLIP)
        quarter[2] = lax.ppermute(quarter[2], "yh", FLIP)
        quarter[3] = lax.ppermute(quarter[3], ("yh", "core"), [(i, 3 - i) for i in range(4)])
        for i, d in enumerate(group):
            done[d] = [q[i] for q in quarter]
    n = lax.axis_size("z")
    out = jnp.stack([jnp.stack(done[d if d <= n // 2 else d - n]) for d in range(n)])
    out = jnp.where(core == 1, out[:, jnp.array([1, 0, 3, 2])], out)
    out = jnp.where(yh == 1, out[:, jnp.array([2, 3, 0, 1])], out)
    out = jnp.concatenate([out, out], axis=0)
    out = lax.dynamic_slice_in_dim(out, (n - z) % n, n, 0)
    return out.reshape(n * 4, 1, tile, rows)


def solution(mesh):
    split = Mesh(mesh.devices.reshape(8, 2, 2, 2, 4), (*SAMP, *SNP))
    return jax.shard_map(
        body,
        mesh=split,
        in_specs=(P(SAMP, SNP), P(SAMP, SNP)),
        out_specs=P(None, SNP, None, SAMP),
        check_vma=False,
    )
```

```python
import jax
import jax.numpy as jnp
from jax import lax
from jax.experimental import pallas as pl
from jax.experimental.pallas import tpu as pltpu
from jax.sharding import Mesh, PartitionSpec as P


var_floor = 0.1
SAMP = ("z", "yh", "core")
SNP = ("yl", "x")
OWNERS = ("yh", "core", "x")
FLIP = [(0, 1), (1, 0)]
NEAR = (0, 1, -1, 2, -2)
FAR = (3, -3, 4)


def from_everyone(x, axis):
    devices = lax.axis_size(axis)
    return lax.all_to_all(jnp.broadcast_to(x[None], (devices, *x.shape)), axis, 0, 0, tiled=True)


def shift(x, axis, by):
    n = lax.axis_size(axis)
    return lax.ppermute(x, axis, [(i, (i + by) % n) for i in range(n)])


def scale(genotypes, observed):
    present = observed.astype(jnp.float32)
    alt_local = jnp.sum(present * genotypes, axis=0)
    call_local = jnp.sum(present, axis=0)
    snps = alt_local.shape[0]
    total = jnp.sum(from_everyone(jnp.concatenate([alt_local, call_local]), SAMP), axis=0)
    alt_sum, call_sum = total[:snps], total[snps:]
    frequency = alt_sum / (2.0 * jnp.maximum(call_sum, 1.0))
    variance = jnp.maximum(2.0 * frequency * (1.0 - frequency), var_floor)
    return (present * (genotypes - 2.0 * frequency) * lax.rsqrt(variance)).astype(jnp.bfloat16)


def flip_y(x, yh, yl):
    pairs = [(h * 2 + l, (h ^ yh) * 2 + (l ^ yl)) for h in range(2) for l in range(2)]
    return lax.ppermute(x, ("yh", "yl"), pairs)


def flip_core(x):
    return lax.ppermute(x, "core", FLIP)


def ring(streams):
    got = {0: list(streams)}
    n = lax.axis_size("z")
    for by in range(1, n // 2 + 1):
        for s in (0, 1):
            if by < n // 2 or s == 0:
                got.setdefault(-by, [None, None])[s] = shift(got[1 - by][s], "z", 1)
            if by < n // 2 or s == 1:
                got.setdefault(by, [None, None])[s] = shift(got[by - 1][s], "z", -1)
    far = n // 2
    last = got.pop(-far)
    got[far][0] = last[0]
    return got


def products(blocks, tiles, at, classes, owner_first):
    count, owners = len(blocks), len(tiles)
    rows, tile_cols = blocks[0][0].shape[0], tiles[0][0].shape[0]
    tile = rows // classes
    shape = (owners, classes, count, tile, tile_cols) if owner_first else (classes, owners, count, tile, tile_cols)

    def kernel(at_ref, *refs):
        left, right, out = refs[:2 * count], refs[2 * count:-1], refs[-1]
        own = jnp.concatenate([r[...] for r in left[0::2]], axis=0)
        partner = jnp.concatenate([r[...] for r in left[1::2]], axis=0)
        contract = (((1,), (1,)), ((), ()))
        for b in range(owners):
            part = lax.dot_general(own, right[2 * b][...], contract, preferred_element_type=jnp.float32)
            part += lax.dot_general(partner, right[2 * b + 1][...], contract, preferred_element_type=jnp.float32)
            part = part.reshape(count, classes, tile, tile_cols)
            slot = at_ref[0] ^ b
            for i in range(count):
                if owner_first:
                    out[slot, :, i] = part[i]
                else:
                    out[:, slot, i] = part[i]

    vmem = pl.BlockSpec(memory_space=pltpu.VMEM)
    flat = [t for pair in (*blocks, *tiles) for t in pair]
    return pl.pallas_call(
        kernel,
        out_shape=jax.ShapeDtypeStruct(shape, jnp.float32),
        in_specs=[pl.BlockSpec(memory_space=pltpu.SMEM)] + [vmem] * len(flat),
        out_specs=vmem,
        name="products",
    )(at.reshape(1), *flat)


def body(genotypes, observed):
    z, yh, core, yl, _ = (lax.axis_index(a) for a in ("z", "yh", "core", "yl", "x"))
    rows, snps = genotypes.shape
    classes = lax.axis_size("x")
    tile = rows // lax.axis_size(SNP)
    n = lax.axis_size("z")
    half = rows // 2
    scaled = scale(genotypes, observed)
    mine = lax.dynamic_slice_in_dim(scaled, yl * half, half, 0)
    theirs = lax.dynamic_slice_in_dim(scaled, (1 - yl) * half, half, 0)
    pair_mine = flip_y(theirs, 0, 1)
    pair_other = flip_y(mine, 0, 1)
    held = ring((mine, pair_mine))
    at = yh * 2 + core
    pair = jnp.concatenate([pair_mine, pair_mine], axis=0)
    pair = lax.dynamic_update_slice_in_dim(pair, pair_other, (1 - yl) * half, 0)
    across = flip_y(scaled, 1, 0)
    across_pair = flip_y(scaled, 1, 1)
    tiles = [
        (scaled, pair),
        (flip_core(scaled), flip_core(pair)),
        (across, across_pair),
        (flip_core(across), flip_core(across_pair)),
    ]
    unit = 2.0 / (snps * lax.axis_size(SNP))
    out = jnp.zeros((n, 4, tile, rows), jnp.float32)

    near = products([held[d] for d in NEAR], tiles, at, classes, False)
    near = (near * 0.5).astype(jnp.float16)
    near = lax.all_to_all(near, "x", 0, 0, tiled=True)
    near = jnp.sum(near.astype(jnp.float32), axis=0) * unit
    far = products([held[d] for d in FAR], tiles, at, classes, True)
    far = (far * 0.5).astype(jnp.float16).reshape(4 * classes, len(FAR), tile, rows)
    far = lax.all_to_all(far, OWNERS, 0, 0, tiled=True)
    far = jnp.sum(far.reshape(4, classes, len(FAR), tile, rows).astype(jnp.float32), axis=1) * unit

    def owned(b):
        return lax.dynamic_index_in_dim(near, at ^ b, 0, keepdims=True)

    pieces = [owned(0), flip_core(owned(1))]
    pieces.append(lax.ppermute(owned(2), "yh", FLIP))
    pieces.append(lax.ppermute(owned(3), ("yh", "core"), [(i, 3 - i) for i in range(4)]))
    merged = jnp.zeros((4, len(NEAR), tile, rows), jnp.float32)
    for b in range(4):
        merged = lax.dynamic_update_slice(merged, pieces[b], (at ^ b, 0, 0, 0))
    for group, part in ((NEAR, merged), (FAR, far)):
        for i, d in enumerate(group):
            out = lax.dynamic_update_slice(out, part[None, :, i], (lax.rem(z + d + n, n), 0, 0, 0))
    return out.reshape(n * 4, 1, tile, rows)


def solution(mesh):
    split = Mesh(mesh.devices.reshape(8, 2, 2, 2, 4), (*SAMP, *SNP))
    return jax.shard_map(
        body,
        mesh=split,
        in_specs=(P(SAMP, SNP), P(SAMP, SNP)),
        out_specs=P(None, SNP, None, SAMP),
        check_vma=False,
    )
```
